256 devices in a mesh: slab: 2 (over z), row: 128 (over y, x, core).
Axes of the slice: x: 8, y: 8, z: 2, core: 2. Of those that a mesh axis runs over, the one named last changes fastest.
The devices are a block of a 8x8x16 slice.
Arguments:
- raw_echo: float32 [2, 8192, 16384], P(None, 'slab', 'row'), parts along dimension 1, may hold values from -6 to 6
- centroid: int32 [64], P('slab'), parts along dimension 0, may hold values from 0 to 16383
- shifts: int32 [64], P('slab'), parts along dimension 0, may hold values from 0 to 12, as said below
- chirp_rate: float32 [8192], P(('slab', 'row')), parts along dimension 0, may hold values from 50 to 400
Outputs:
- focused_image: float32 [2, 8192, 16384], P(None, ('slab', 'row')), parts along dimension 1
The draws below stay inside these ranges and needn't reach their ends.
There are 2 independent parts, one for each index of `slab`. The reference program is written for one: setup_inputs(seed, part) draws one part's arguments, and reference() takes and returns one part's arrays. A program takes and returns all parts, laid end to end along the dimension named above; each array names one. Nothing has to cross between parts.
Inputs may be any that keep to these rules, and one draw needn't show every extreme that they name: `shifts`: range migration of each block in range bins; some block reaches 12 in every draw.
All inputs are finite; a program needn't handle non-finite values.
Results may differ from the reference program's by a relative error of at most 0.0003.
Values sent between devices are 32-bit elements; how exact they have to be, the bound alone decides.
No kernel may reach another device: no remote copies, remote signals or barrier semaphores. Data moves between devices by JAX's collectives and lax.ppermute only.
A program may use at most 128 MiB of HBM per device.

```python
import math
import jax
import jax.numpy as jnp
from jax import lax

PULSES = 16384
RANGE = 4096
BLOCK = 128
MAXSHIFT = 12
TAPS = 4


def slab_plan(key):
    block_count = RANGE // BLOCK
    block_ids = jnp.arange(block_count, dtype=jnp.int32)
    chosen = jax.random.randint(jax.random.fold_in(key, 23), (), 0, block_count, dtype=jnp.int32)
    shift_draw = jax.random.randint(jax.random.fold_in(key, 11), (block_count,), 0, MAXSHIFT + 1, dtype=jnp.int32)
    shift_values = jnp.where(block_ids == chosen, MAXSHIFT, shift_draw)
    center_draw = jax.random.randint(jax.random.fold_in(key, 37), (block_count,), 0, PULSES, dtype=jnp.int32)
    edge_center = 8 * jax.random.randint(jax.random.fold_in(key, 41), (), 0, PULSES // 8, dtype=jnp.int32) + 4
    centers = jnp.where(block_ids == chosen, edge_center, center_draw)
    return (centers, shift_values, chosen, edge_center)


def draw_centroid(key, part):
    return slab_plan(key)[0]


def draw_shifts(key, part):
    return slab_plan(key)[1]


def draw_raw_echo(key, part):
    centers, shift_values, chosen, edge_center = slab_plan(key)
    noise_key = jax.random.fold_in(key, 53)
    noise = jax.random.truncated_normal(noise_key, -6.0, 6.0, (2, RANGE, PULSES), jnp.float32)
    quarter = BLOCK // 4
    pulse_index = jnp.arange(PULSES, dtype=jnp.int32)
    edge_bin = (edge_center + PULSES // 2) % PULSES
    first_offset = PULSES // 16 + jax.random.randint(jax.random.fold_in(key, 61), (), 0, PULSES // 32 + 1, dtype=jnp.int32)
    candidates = first_offset + jnp.arange(PULSES // 16, dtype=jnp.int32)
    ratio = candidates.astype(jnp.float32) / PULSES
    scaled = 32.0 * MAXSHIFT * 4.0 * ratio * ratio
    offset_score = jnp.abs(scaled - jnp.floor(scaled) - 0.5)
    distance = candidates[jnp.argmin(offset_score)]
    sign_draw = jnp.where(jax.random.bernoulli(jax.random.fold_in(key, 67)), 1, -1).astype(jnp.int32)
    table_bin = (edge_center + sign_draw * distance) % PULSES
    row_local = jnp.arange(2 * quarter, dtype=jnp.int32)
    bins = jnp.where(row_local < quarter, edge_bin, table_bin)
    edge_phases = jax.random.uniform(jax.random.fold_in(key, 71), (2 * quarter,), jnp.float32, 0.0, 2.0 * math.pi)
    table_phase = jax.random.uniform(jax.random.fold_in(key, 79), (), jnp.float32, 0.0, 2.0 * math.pi)
    alternating = math.pi * (row_local % 2).astype(jnp.float32)
    row_phase = jnp.where(row_local < quarter, edge_phases, table_phase + alternating)
    cycles = (bins[:, None] * pulse_index[None, :] % PULSES).astype(jnp.float32)
    angles = 2.0 * math.pi / PULSES * cycles + row_phase[:, None]
    small_noise = jnp.clip(0.3 * jax.random.normal(jax.random.fold_in(key, 83), (2, 2 * quarter, PULSES), jnp.float32), -1.0, 1.0)
    tones = 5.0 * jnp.stack([jnp.cos(angles), jnp.sin(angles)]) + small_noise
    anchor = jnp.zeros((), jnp.int32)
    start_row = (chosen * BLOCK).astype(jnp.int32)
    return lax.dynamic_update_slice(noise, tones.astype(jnp.float32), (anchor, start_row, anchor))


def block_levels(own_key, dims, pieces, smallest, high):
    factor_of = 1.0
    for dim, blocks in pieces:
        steps = jax.random.uniform(jax.random.fold_in(jax.random.fold_in(own_key, 6), dim), (blocks,), jnp.float32, smallest / len(pieces), high / len(pieces))
        factor_of = factor_of * jnp.repeat(jnp.exp(steps), dims[dim] // blocks).reshape((-1,) + (1,) * (len(dims) - 1 - dim))
    return factor_of


def setup_inputs(seed: int = 0, part: int = 0) -> dict:
    key_of = jax.random.split(jax.random.key(seed), 5)
    part_splits = jax.random.split(jax.random.fold_in(key_of[4], part), 5)
    raw_echo = draw_raw_echo(jax.random.fold_in(jax.random.fold_in(key_of[4], part), 71), part)
    centroid = draw_centroid(jax.random.fold_in(jax.random.fold_in(key_of[4], part), 71), part)
    shifts = draw_shifts(jax.random.fold_in(jax.random.fold_in(key_of[4], part), 71), part)
    chirp_rate = jnp.clip(jnp.exp(math.log(400.0) - 2.0794415 * jax.random.uniform(part_splits[3], (RANGE,), jnp.float32) ** block_levels(part_splits[3], (RANGE,), ((0, 128),), -0.2, 0.2)), 50.0, 400.0)
    return {"raw_echo": raw_echo, "centroid": centroid, "shifts": shifts, "chirp_rate": chirp_rate}


def relative_doppler(center_bin):
    doppler_bins = jnp.arange(PULSES, dtype=jnp.int32)
    wrapped = (doppler_bins - center_bin + PULSES // 2) % PULSES - PULSES // 2
    return wrapped.astype(jnp.float32) / PULSES


def kernel(offsets):
    inside = jnp.abs(offsets) < TAPS
    tapering = jnp.cos(math.pi * offsets / (2.0 * TAPS))
    return jnp.where(inside, jnp.sinc(offsets) * tapering * tapering, 0.0)


def reference(raw_echo, centroid, shifts, chirp_rate):
    lower_rim = TAPS - 1
    upper_rim = MAXSHIFT + TAPS - 1
    padded = jnp.pad(raw_echo, ((0, 0), (lower_rim, upper_rim), (0, 0)))
    extent = BLOCK + lower_rim + upper_rim

    def one_block(block_index):
        first_row = (block_index * BLOCK).astype(jnp.int32)
        anchor = jnp.zeros((), jnp.int32)
        window_rows = lax.dynamic_slice(padded, (anchor, first_row, anchor), (2, extent, PULSES))
        spectrum = jnp.fft.fft(window_rows[0] + 1j * window_rows[1], axis=-1)
        relative = relative_doppler(centroid[block_index])
        migration = shifts[block_index].astype(jnp.float32) * 4.0 * relative * relative
        migrated = kernel(-lower_rim - migration)[None, :] * spectrum[0:BLOCK]
        for offset in range(1 - lower_rim, upper_rim + 1):
            weight = kernel(offset - migration)
            start_row = offset + lower_rim
            migrated = migrated + weight[None, :] * spectrum[start_row:start_row + BLOCK]
        block_rates = lax.dynamic_slice(chirp_rate, (first_row,), (BLOCK,))
        window = 0.54 + 0.46 * jnp.cos(2.0 * math.pi * relative)
        phase_angle = math.pi * block_rates[:, None] * (relative * relative)[None, :]
        focused = migrated * window[None, :] * (jnp.cos(phase_angle) - 1j * jnp.sin(phase_angle))
        picture = jnp.fft.ifft(focused, axis=-1)
        return jnp.stack([jnp.real(picture), jnp.imag(picture)]).astype(jnp.float32)

    blocks = lax.map(one_block, jnp.arange(RANGE // BLOCK, dtype=jnp.int32))
    return jnp.transpose(blocks, (1, 0, 2, 3)).reshape(2, RANGE, PULSES)
```

```python
import math

import jax
import jax.numpy as jnp
import numpy as np
from jax import lax
from jax.experimental import pallas as pl
from jax.experimental.pallas import tpu as pltpu
from jax.sharding import PartitionSpec as P

FACTOR = 128
PULSES = 16384
BLOCK = 128
MAXSHIFT = 12
TAPS = 4
LOWER = TAPS - 1
UPPER = MAXSHIFT + TAPS - 1
COUNT = LOWER + UPPER + 1
PITCH = 72


def from_behind(shard, axis, by):
    devices = lax.axis_size(axis)
    pairs = [(i, i + by) for i in range(devices) if 0 <= i + by < devices]
    return lax.ppermute(shard, axis, pairs)


def split(values):
    high = values.astype(jnp.bfloat16)
    low = (values - high.astype(jnp.float32)).astype(jnp.bfloat16)
    return high, low


def tables():
    index = np.arange(FACTOR)
    product = index[:, None] * index[None, :]
    angle = 2.0 * np.pi / FACTOR * (product % FACTOR)
    c, s = np.cos(angle), np.sin(angle)
    left = np.block([[c, s], [-s, c]]).astype(np.float32)
    right = np.block([[c, -s], [s, c]]).astype(np.float32)
    twist = 2.0 * np.pi / PULSES * product
    pieces = []
    for matrix in (left, right):
        high = matrix.astype(jnp.bfloat16)
        low = (matrix - high.astype(np.float32)).astype(jnp.bfloat16)
        pieces += [jnp.asarray(high), jnp.asarray(low)]
    return pieces + [jnp.asarray(np.cos(twist), jnp.float32), jnp.asarray(np.sin(twist), jnp.float32)]


def dot3(a, b):
    def dot(x, y):
        return jnp.dot(x, y, preferred_element_type=jnp.float32)

    return dot(a[0], b[0]) + (dot(a[0], b[1]) + dot(a[1], b[0]))


def stack2(a, b, c, d):
    return jnp.concatenate([jnp.concatenate([a, b], axis=1), jnp.concatenate([c, d], axis=1)], axis=0)


def forward_body(x, lh, ll, rh, rl, tc, ts, spec, up, down, xs, sems):
    group = pl.program_id(0)
    groups = pl.num_programs(0)
    view = xs.reshape(FACTOR, PITCH, FACTOR)

    def fetch(g, part):
        rows = pl.ds(pl.multiple_of(8 * g, 8), 8)
        target = pl.ds(pl.multiple_of(32 * part + 8 * g, 8), 8)
        return pltpu.make_async_copy(x.at[:, part, rows, :], view.at[:, target, :], sems.at[g, part])

    @pl.when(group == 0)
    def _():
        for g in range(4):
            for part in range(2):
                fetch(g, part).start()

    for part in range(2):
        fetch(group, part).wait()

    def load(part, row):
        return xs[pl.ds(32 * part + row, FACTOR, stride=PITCH), :]

    def pair(row):
        data = stack2(load(0, row), load(0, row + 1), load(1, row), load(1, row + 1))
        first = dot3((lh[...], ll[...]), split(data))
        c, s = tc[...], ts[...]
        halves = []
        for i in range(2):
            fr = first[:FACTOR, FACTOR * i : FACTOR * (i + 1)]
            fi = first[FACTOR:, FACTOR * i : FACTOR * (i + 1)]
            halves.append((fr * c + fi * s, fi * c - fr * s))
        turned = stack2(halves[0][0], halves[0][1], halves[1][0], halves[1][1])
        return dot3(split(turned), (rh[...], rl[...]))

    def quad(step, carry):
        for half in range(2):
            local = 4 * step + 2 * half
            result = pair(8 * group + local)
            for i in range(2):
                for part in range(2):
                    value = result[FACTOR * i : FACTOR * (i + 1), FACTOR * part : FACTOR * (part + 1)]
                    spec[local + i, part] = value
                    row = 8 * group + local + i

                    @pl.when(row < UPPER)
                    def _():
                        up[row, part] = value

                    @pl.when(row >= 8 * groups - LOWER)
                    def _():
                        down[row - (8 * groups - LOWER), part] = value

        return carry

    lax.fori_loop(0, 2, quad, 0)


def forward(x, consts):
    rows = x.shape[2]
    whole = lambda shape: pl.BlockSpec(shape, lambda g: (0,) * len(shape))
    plane = (FACTOR, FACTOR)
    return pl.pallas_call(
        forward_body,
        grid=(rows // 8,),
        in_specs=[pl.BlockSpec(memory_space=pl.ANY)] + [whole((256, 256))] * 4 + [whole(plane)] * 2,
        out_specs=[
            pl.BlockSpec((8, 2) + plane, lambda g: (g, 0, 0, 0)),
            whole((UPPER, 2) + plane),
            whole((LOWER, 2) + plane),
        ],
        out_shape=[jax.ShapeDtypeStruct((n, 2) + plane, jnp.float32) for n in (rows, UPPER, LOWER)],
        scratch_shapes=[pltpu.VMEM((FACTOR * PITCH, FACTOR), jnp.float32), pltpu.SemaphoreType.DMA((4, 2))],
        compiler_params=pltpu.CompilerParams(vmem_limit_bytes=40 << 20),
        cost_estimate=pl.CostEstimate(flops=3 * 2 * 2 * 2 * 256 * 256 * 2048, bytes_accessed=10 << 20, transcendentals=0),
        name="forward",
    )(x, *consts)


def focus_body(spec, above, below, weights, chirp, lh, ll, rh, rl, tc, ts, out, ext, work, sems):
    group = pl.program_id(0)
    rows = spec.shape[0]
    copies = [
        pltpu.make_async_copy(spec, ext.at[pl.ds(LOWER, rows)], sems.at[0]),
        pltpu.make_async_copy(below, ext.at[pl.ds(0, LOWER)], sems.at[1]),
        pltpu.make_async_copy(above, ext.at[pl.ds(LOWER + rows, UPPER)], sems.at[2]),
    ]

    @pl.when(group == 0)
    def _():
        for copy in copies:
            copy.start()
        for copy in copies:
            copy.wait()

    view = out.reshape(2 * FACTOR * 8, FACTOR)

    def quad(step, carry):
        local = 4 * step
        base = 8 * group + local

        def tile(t, inner):
            sub = pl.ds(pl.multiple_of(8 * t, 8), 8)
            w = [weights[k, sub, :] for k in range(COUNT)]
            sums = [[None, None] for _ in range(4)]
            for j in range(COUNT + 3):
                values = [ext[base + j, part, sub, :] for part in range(2)]
                for i in range(4):
                    if 0 <= j - i < COUNT:
                        for part in range(2):
                            term = w[j - i] * values[part]
                            sums[i][part] = term if sums[i][part] is None else sums[i][part] + term
            for i in range(4):
                re, im = sums[i]
                c, s = chirp[local + i, 0, sub, :], chirp[local + i, 1, sub, :]
                target = pl.ds(pl.multiple_of(FACTOR * i + 8 * t, 8), 8)
                work[target, :FACTOR] = re * c + im * s
                work[target, FACTOR:] = im * c - re * s
            return inner

        lax.fori_loop(0, FACTOR // 8, tile, 0)
        for half in range(2):
            data = work[256 * half : 256 * (half + 1), :]
            first = dot3(split(data), (lh[...], ll[...]))
            c, s = tc[...], ts[...]
            halves = []
            for i in range(2):
                fr = first[FACTOR * i : FACTOR * (i + 1), :FACTOR]
                fi = first[FACTOR * i : FACTOR * (i + 1), FACTOR:]
                halves.append((fr * c - fi * s, fi * c + fr * s))
            turned = stack2(halves[0][0], halves[1][0], halves[0][1], halves[1][1])
            result = dot3((rh[...], rl[...]), split(turned))
            for i in range(2):
                for part in range(2):
                    value = result[FACTOR * part : FACTOR * (part + 1), FACTOR * i : FACTOR * (i + 1)]
                    view[pl.ds(FACTOR * 8 * part + local + 2 * half + i, FACTOR, stride=8), :] = value
        return carry

    lax.fori_loop(0, 2, quad, 0)


def focus(spec, above, below, weights, chirp, consts):
    rows = spec.shape[0]
    whole = lambda shape: pl.BlockSpec(shape, lambda g: (0,) * len(shape))
    plane = (FACTOR, FACTOR)
    anywhere = pl.BlockSpec(memory_space=pl.ANY)
    return pl.pallas_call(
        focus_body,
        grid=(rows // 8,),
        in_specs=[anywhere] * 3
        + [whole((COUNT,) + plane), pl.BlockSpec((8, 2) + plane, lambda g: (g, 0, 0, 0))]
        + [whole((256, 256))] * 4
        + [whole(plane)] * 2,
        out_specs=pl.BlockSpec((2, None, FACTOR, 8, FACTOR), lambda g: (0, g, 0, 0, 0)),
        out_shape=jax.ShapeDtypeStruct((2, rows // 8, FACTOR, 8, FACTOR), jnp.float32),
        scratch_shapes=[
            pltpu.VMEM((rows + LOWER + UPPER, 2) + plane, jnp.float32),
            pltpu.VMEM((512, 256), jnp.float32),
            pltpu.SemaphoreType.DMA((3,)),
        ],
        compiler_params=pltpu.CompilerParams(vmem_limit_bytes=40 << 20),
        cost_estimate=pl.CostEstimate(flops=3 * 2 * 2 * 2 * 256 * 256 * 2048, bytes_accessed=16 << 20, transcendentals=0),
        name="focus",
    )(spec, above, below, weights, chirp, *consts)


def spectral_tables(centroid, shifts, chirp_rate, own_rows):
    block = lax.axis_index("row") * own_rows // BLOCK
    chosen = block == jnp.arange(centroid.shape[0], dtype=jnp.int32)
    center = jnp.sum(jnp.where(chosen, centroid, 0))
    distance = jnp.sum(jnp.where(chosen, shifts, 0))
    index = jnp.arange(FACTOR, dtype=jnp.int32)
    bins = index[:, None] + FACTOR * index[None, :]
    wrapped = (bins - center + PULSES // 2) % PULSES - PULSES // 2
    relative = wrapped.astype(jnp.float32) / PULSES
    migration = distance.astype(jnp.float32) * 4.0 * relative * relative
    nearest = jnp.round(migration)
    sine = jnp.sin(math.pi * (migration - nearest)) / math.pi
    odd = nearest.astype(jnp.int32) % 2
    slow_cos, slow_sin = jnp.cos(math.pi / 4.0 * migration), jnp.sin(math.pi / 4.0 * migration)
    weights = []
    for offset in range(-LOWER, UPPER + 1):
        away = offset - migration
        sign = jnp.where((odd + offset) % 2 == 0, -1.0, 1.0)
        ratio = jnp.where(away == 0.0, 1.0, sign * sine / jnp.where(away == 0.0, 1.0, away))
        turn = math.pi / 4.0 * offset
        taper = 0.5 + 0.5 * (math.cos(turn) * slow_cos + math.sin(turn) * slow_sin)
        weights.append(jnp.where(jnp.abs(away) < TAPS, ratio * taper, 0.0))
    window = (0.54 + 0.46 * jnp.cos(2.0 * math.pi * relative)) / PULSES
    phase = math.pi * chirp_rate[:, None, None] * (relative * relative)
    return jnp.stack(weights), jnp.stack([window * jnp.cos(phase), window * jnp.sin(phase)], axis=1)


def per_device(raw_echo, centroid, shifts, chirp_rate):
    devices = lax.axis_size("row")
    own_rows = raw_echo.shape[1] // devices
    blocks = raw_echo.reshape(2, devices, own_rows, raw_echo.shape[2]).transpose(1, 0, 2, 3)
    received = lax.all_to_all(blocks, "row", split_axis=0, concat_axis=0, tiled=True)
    weights, chirp = spectral_tables(centroid, shifts, chirp_rate, own_rows)
    lh, ll, rh, rl, tc, ts = tables()
    spec, up, down = forward(received, (lh, ll, rh, rl, tc, ts))
    above = from_behind(up, "row", -1)
    below = from_behind(down, "row", 1)
    image = focus(spec, above, below, weights, chirp, (lh, ll, rh, rl, tc, ts))
    return image.transpose(0, 1, 3, 2, 4).reshape(2, own_rows, PULSES)


def solution(mesh):
    return jax.shard_map(
        per_device,
        mesh=mesh,
        in_specs=(P(None, "slab", "row"), P("slab"), P("slab"), P(("slab", "row"))),
        out_specs=P(None, ("slab", "row"), None),
        check_vma=False,
    )
```

```python
import math

import jax
import jax.numpy as jnp
from jax import lax
from jax.experimental import pallas as pl
from jax.experimental.pallas import tpu as pltpu
from jax.sharding import PartitionSpec as P

FACTOR = 128
PULSES = 16384
BLOCK = 128
MAXSHIFT = 12
TAPS = 4
LOWER = TAPS - 1
UPPER = MAXSHIFT + TAPS - 1
PITCH = 72
TILES = FACTOR // 8
PLANE = (FACTOR, FACTOR)
TABLE = (2 * FACTOR, 2 * FACTOR)


def edge(tile):
    return min(tile, TILES - 1 - tile)


def last_tap(tile):
    return math.ceil(4 * MAXSHIFT * ((8 - edge(tile)) / TILES) ** 2) + TAPS - 1


def tap_count(tile):
    near, far = (7 - edge(tile)) / TILES, (8 - edge(tile)) / TILES
    return max(math.ceil(4 * s * far**2) - math.floor(4 * s * near**2) + 2 * TAPS - 1 for s in range(MAXSHIFT + 1))


def side_tiles(row):
    return sum(4 * MAXSHIFT * ((8 - e) / TILES) ** 2 > row - LOWER for e in range(TILES // 2))


COUNTS = [tap_count(t) for t in range(TILES)]
LASTS = [last_tap(t) for t in range(TILES)]
SIDES = [side_tiles(j) for j in range(UPPER)]
STARTS = [16 * sum(SIDES[:j]) for j in range(UPPER + 1)]


def from_behind(shard, axis, by):
    devices = lax.axis_size(axis)
    pairs = [(i, i + by) for i in range(devices) if 0 <= i + by < devices]
    return lax.ppermute(shard, axis, pairs)


def split(values):
    high = values.astype(jnp.bfloat16)
    low = (values - high.astype(jnp.float32)).astype(jnp.bfloat16)
    return high, low


def stack2(a, b, c, d):
    return jnp.concatenate([jnp.concatenate([a, b], axis=1), jnp.concatenate([c, d], axis=1)], axis=0)


def multiply(table, data, across):
    dims = (((1,), (1 if across else 0,)), ((), ()))

    def dot(x, y):
        return lax.dot_general(x, y, dims, preferred_element_type=jnp.float32)

    high, low = split(data)
    return dot(table[0][...], high) + (dot(table[0][...], low) + dot(table[1][...], high))


def quarters(values):
    n = FACTOR
    return values[:n, :n], values[:n, n:], values[n:, :n], values[n:, n:]


def transform_pair(re0, re1, im0, im1, first, twist, second, sign):
    a = multiply(first, stack2(re0, re1, im0, im1), False)
    r0, r1, i0, i1 = quarters(a)
    c, s = twist[0][...], twist[1][...]
    if sign < 0:
        turned = stack2(r0 * c + i0 * s, i0 * c - r0 * s, r1 * c + i1 * s, i1 * c - r1 * s)
    else:
        turned = stack2(r0 * c - i0 * s, i0 * c + r0 * s, r1 * c - i1 * s, i1 * c + r1 * s)
    return quarters(multiply(second, turned, True))


def fetcher(x, xs, sems):
    view = xs.reshape(FACTOR, PITCH, FACTOR)

    def fetch(g, part):
        rows = pl.ds(pl.multiple_of(8 * g, 8), 8)
        target = pl.ds(pl.multiple_of(32 * part + 8 * g, 8), 8)
        return pltpu.make_async_copy(x.at[:, part, rows, :], view.at[:, target, :], sems.at[g, part])

    return fetch


def forward_pair(xs, row, tables):
    def load(part, r):
        return xs[pl.ds(32 * part + r, FACTOR, stride=PITCH), :]

    return transform_pair(
        load(0, row), load(0, row + 1), load(1, row), load(1, row + 1), tables[0:2], tables[2:4], tables[4:6], -1
    )


def halo_body(*refs):
    x, up_tables, down_tables = refs[0], refs[1:7], refs[7:13]
    up, down, xs, sems = refs[13:]
    fetch = fetcher(x, xs, sems)
    for g in (0, 1, 3):
        for part in range(2):
            fetch(g, part).start()
    for g in (0, 1, 3):
        for part in range(2):
            fetch(g, part).wait()
        for row in range(8 * g, 8 * g + 8, 2):
            if g < 3:
                re0, re1, im0, im1 = forward_pair(xs, row, up_tables)
                for r, re, im in ((row, re0, im0), (row + 1, re1, im1)):
                    if r < UPPER:
                        start, size = STARTS[r], 8 * SIDES[r]
                        for part, value in enumerate((re, im)):
                            up[part, start : start + size, :] = value[:size]
                            up[part, start + size : start + 2 * size, :] = value[FACTOR - size :]
            elif row + 1 >= 32 - LOWER:
                re0, re1, im0, im1 = forward_pair(xs, row, down_tables)
                for r, re, im in ((row, re0, im0), (row + 1, re1, im1)):
                    if r >= 32 - LOWER:
                        down[r - 32 + LOWER, 0] = re
                        down[r - 32 + LOWER, 1] = im


def halo(x, up_tables, down_tables):
    return pl.pallas_call(
        halo_body,
        in_specs=[pl.BlockSpec(memory_space=pl.ANY)] + [pl.BlockSpec(memory_space=pltpu.VMEM)] * 12,
        out_shape=[
            jax.ShapeDtypeStruct((2, STARTS[-1], FACTOR), jnp.float32),
            jax.ShapeDtypeStruct((LOWER, 2) + PLANE, jnp.float32),
        ],
        scratch_shapes=[pltpu.VMEM((FACTOR * PITCH, FACTOR), jnp.float32), pltpu.SemaphoreType.DMA((4, 2))],
        compiler_params=pltpu.CompilerParams(vmem_limit_bytes=16 << 20),
        cost_estimate=pl.CostEstimate(flops=5 << 30, bytes_accessed=5 << 20, transcendentals=0),
        name="halo",
    )(x, *up_tables, *down_tables)


def forward_body(*refs):
    x, tables = refs[0], refs[1:7]
    spec, xs, sems = refs[7:]
    group = pl.program_id(0)
    fetch = fetcher(x, xs, sems)

    @pl.when(group == 0)
    def _():
        for g in range(4):
            for part in range(2):
                fetch(g, part).start()

    for part in range(2):
        fetch(group, part).wait()
    for local in range(0, 8, 2):
        re0, re1, im0, im1 = forward_pair(xs, 8 * group + local, tables)
        spec[local, 0] = re0
        spec[local + 1, 0] = re1
        spec[local, 1] = im0
        spec[local + 1, 1] = im1


def whole(shape):
    return pl.BlockSpec(shape, lambda *_: (0,) * len(shape))


def forward(x, tables):
    rows = x.shape[2]
    return pl.pallas_call(
        forward_body,
        grid=(rows // 8,),
        in_specs=[pl.BlockSpec(memory_space=pl.ANY)] + [whole(t.shape) for t in tables],
        out_specs=pl.BlockSpec((8, 2) + PLANE, lambda g: (g, 0, 0, 0)),
        out_shape=jax.ShapeDtypeStruct((rows, 2) + PLANE, jnp.float32),
        scratch_shapes=[pltpu.VMEM((FACTOR * PITCH, FACTOR), jnp.float32), pltpu.SemaphoreType.DMA((4, 2))],
        compiler_params=pltpu.CompilerParams(vmem_limit_bytes=16 << 20),
        cost_estimate=pl.CostEstimate(flops=8 << 30, bytes_accessed=8 << 20, transcendentals=0),
        name="forward",
    )(x, *tables)


def focus_rows(ext, taps, weights, chirp, tables, view, base, local):
    tiles = [[[], []] for _ in range(4)]
    for t in range(TILES):
        sub = slice(8 * t, 8 * t + 8)
        start = base + local + taps[t] + LOWER
        w = [weights[k, sub, :] for k in range(COUNTS[t])]
        sums = [[None, None] for _ in range(4)]
        for j in range(COUNTS[t] + 3):
            values = [ext[start + j, part, sub, :] for part in range(2)]
            for i in range(4):
                if 0 <= j - i < COUNTS[t]:
                    for part in range(2):
                        term = w[j - i] * values[part]
                        sums[i][part] = term if sums[i][part] is None else sums[i][part] + term
        for i in range(4):
            re, im = sums[i]
            c, s = chirp[local + i, 0, sub, :], chirp[local + i, 1, sub, :]
            tiles[i][0].append(re * c + im * s)
            tiles[i][1].append(im * c - re * s)
    planes = [[jnp.concatenate(part, axis=0) for part in row] for row in tiles]
    for i in (0, 2):
        (re0, im0), (re1, im1) = planes[i], planes[i + 1]
        re0, re1, im0, im1 = transform_pair(re0, re1, im0, im1, tables[0:2], tables[2:4], tables[4:6], 1)
        for part, r, value in ((0, 0, re0), (0, 1, re1), (1, 0, im0), (1, 1, im1)):
            view[pl.ds(FACTOR * 8 * part + local + i + r, FACTOR, stride=8), :] = value


def inner_body(*refs):
    taps, spec, weights, chirp = refs[:4]
    tables, (out, ext, sems) = refs[4:10], refs[10:]
    first, count = 8 - LOWER, 8 + LOWER + UPPER
    copy = pltpu.make_async_copy(spec.at[pl.ds(first, count)], ext.at[pl.ds(8, count)], sems.at[0])
    copy.start()
    copy.wait()
    view = out.reshape(2 * FACTOR * 8, FACTOR)
    for local in (0, 4):
        focus_rows(ext, taps, weights, chirp, tables, view, 8, local)


def outer_body(*refs):
    taps, spec, up, down, weights, chirp = refs[:6]
    tables, (_, out, ext, sems) = refs[6:12], refs[12:]
    step = pl.program_id(0)
    rows = spec.shape[0]

    @pl.when(step == 0)
    def _():
        copy = pltpu.make_async_copy(spec, ext.at[pl.ds(LOWER, rows)], sems.at[0])
        copy.start()
        for r in range(LOWER):
            ext[r] = down[r]
        for r in range(UPPER):
            start, size = STARTS[r], 8 * SIDES[r]
            for part in range(2):
                ext[LOWER + rows + r, part, :size, :] = up[part, start : start + size, :]
                ext[LOWER + rows + r, part, FACTOR - size :, :] = up[part, start + size : start + 2 * size, :]
        copy.wait()

    view = out.reshape(2 * FACTOR * 8, FACTOR)
    base = 8 * (step + jnp.minimum(step, 1))
    for local in (0, 4):
        focus_rows(ext, taps, weights, chirp, tables, view, base, local)


def focus(group_of, steps, body, taps, operands, kinds, weights, chirp, tables, rows, prior, name):
    chunk = lambda g: (group_of(g), 0, 0, 0)
    image = pl.BlockSpec((2, None, FACTOR, 8, FACTOR), lambda g: (0, group_of(g), 0, 0, 0))
    specs = [pl.BlockSpec(memory_space=pltpu.SMEM)] + kinds + [whole(weights.shape), pl.BlockSpec((8, 2) + PLANE, chunk)]
    specs += [whole(t.shape) for t in tables]
    args = [taps, *operands, weights, chirp, *tables]
    aliases = {}
    if prior is not None:
        aliases = {len(args): 0}
        specs.append(pl.BlockSpec(memory_space=pl.ANY))
        args.append(prior)
    return pl.pallas_call(
        body,
        grid=(steps,),
        in_specs=specs,
        out_specs=image,
        out_shape=jax.ShapeDtypeStruct((2, rows // 8, FACTOR, 8, FACTOR), jnp.float32),
        input_output_aliases=aliases,
        scratch_shapes=[
            pltpu.VMEM((rows + LOWER + UPPER, 2) + PLANE, jnp.float32),
            pltpu.SemaphoreType.DMA((1,)),
        ],
        compiler_params=pltpu.CompilerParams(vmem_limit_bytes=24 << 20),
        cost_estimate=pl.CostEstimate(flops=steps * (3 << 30), bytes_accessed=steps * (4 << 20), transcendentals=0),
        name=name,
    )(*args)


def two_parts(values):
    high = lax.reduce_precision(values, 8, 7)
    return high.astype(jnp.bfloat16), (values - high).astype(jnp.bfloat16)


def turns(product, modulus):
    angle = 2.0 * math.pi / modulus * (product % modulus).astype(jnp.float32)
    return jnp.cos(angle), jnp.sin(angle)


def transform_tables(center, sign):
    start = (center - PULSES // 2) % PULSES
    index = jnp.arange(FACTOR, dtype=jnp.int32)
    fine, coarse = index + start % FACTOR, index + start // FACTOR

    def block(a, b):
        c, s = turns(a[:, None] * b[None, :], FACTOR)
        return two_parts(stack2(c, -sign * s, sign * s, c))

    if sign < 0:
        twist = turns(fine[:, None] * index[None, :], PULSES)
        return [*block(fine, index), *twist, *block(coarse, index)]
    twist = turns(index[:, None] * fine[None, :], PULSES)
    return [*block(index, coarse), *twist, *block(index, fine)]


def spectral_tables(distance, chirp_rate):
    index = jnp.arange(FACTOR, dtype=jnp.int32)
    bins = FACTOR * index[:, None] + index[None, :]
    relative = (bins - PULSES // 2).astype(jnp.float32) / PULSES
    migration = distance.astype(jnp.float32) * 4.0 * relative * relative
    nearness = jnp.array([(7 - edge(t)) ** 2 for t in range(TILES)], jnp.int32)
    latest = jnp.array([LASTS[t] - COUNTS[t] + 1 for t in range(TILES)], jnp.int32)
    taps = jnp.minimum(distance * nearness // (TILES * TILES // 4) - LOWER, latest)
    nearest = jnp.round(migration)
    sine = jnp.sin(math.pi * (migration - nearest)) / math.pi
    quarter = math.pi / TAPS
    offset = jnp.repeat(taps, 8)[None, :, None] + jnp.arange(max(COUNTS), dtype=jnp.int32)[:, None, None]
    away = offset.astype(jnp.float32) - migration
    sign = jnp.where((nearest.astype(jnp.int32) + offset) % 2 == 0, -1.0, 1.0)
    ratio = jnp.where(away == 0.0, 1.0, sign * sine / jnp.where(away == 0.0, 1.0, away))
    inside = jnp.abs(away) < TAPS
    weights = jnp.where(inside, ratio * (0.5 + 0.5 * jnp.cos(quarter * away)), 0.0)
    window = (0.54 + 0.46 * jnp.cos(2.0 * math.pi * relative)) / PULSES
    phase = math.pi * chirp_rate[:, None, None] * (relative * relative)
    return taps, weights, jnp.stack([window * jnp.cos(phase), window * jnp.sin(phase)], axis=1)


def compute(received, exchange, own, below, above, distance, chirp_rate):
    rows = received.shape[2]
    taps, weights, chirp = spectral_tables(distance, chirp_rate)
    inverse = transform_tables(own, 1)
    up, down = halo(received, transform_tables(below, -1), transform_tables(above, -1))
    up, down = exchange(up, down)
    spec = forward(received, transform_tables(own, -1))
    anywhere = pl.BlockSpec(memory_space=pl.ANY)
    image = focus(lambda g: 1, 1, inner_body, taps, [spec], [anywhere], weights, chirp, inverse, rows, None, "inner")
    kinds = [anywhere, whole(up.shape), whole(down.shape)]
    later = lambda g: g + jnp.minimum(g, 1)
    image = focus(later, 3, outer_body, taps, [spec, up, down], kinds, weights, chirp, inverse, rows, image, "outer")
    return image.transpose(0, 1, 3, 2, 4).reshape(2, rows, PULSES)


def per_device(raw_echo, centroid, shifts, chirp_rate):
    devices = lax.axis_size("row")
    own_rows = raw_echo.shape[1] // devices
    blocks = raw_echo.reshape(2, devices, own_rows, raw_echo.shape[2]).transpose(1, 0, 2, 3)
    received = lax.all_to_all(blocks, "row", split_axis=0, concat_axis=0, tiled=True)

    def pick(values, device):
        block = jnp.clip(device, 0, devices - 1) * own_rows // BLOCK
        return jnp.sum(jnp.where(block == jnp.arange(values.shape[0], dtype=jnp.int32), values, 0))

    def exchange(up, down):
        return from_behind(up, "row", -1), from_behind(down, "row", 1)

    device = lax.axis_index("row")
    centers = [pick(centroid, device + by) for by in (0, -1, 1)]
    return compute(received, exchange, *centers, pick(shifts, device), chirp_rate)


def solution(mesh):
    return jax.shard_map(
        per_device,
        mesh=mesh,
        in_specs=(P(None, "slab", "row"), P("slab"), P("slab"), P(("slab", "row"))),
        out_specs=P(None, ("slab", "row"), None),
        check_vma=False,
    )
```

```python
import math

import jax
import jax.numpy as jnp
from jax import lax
from jax.experimental import pallas as pl
from jax.experimental.pallas import tpu as pltpu
from jax.sharding import PartitionSpec as P

FACTOR = 128
PULSES = 16384
BLOCK = 128
MAXSHIFT = 12
TAPS = 4
LOWER = TAPS - 1
UPPER = MAXSHIFT + TAPS - 1
PITCH = 72
TILES = FACTOR // 8
PLANE = (FACTOR, FACTOR)
TABLE = (2 * FACTOR, 2 * FACTOR)


def edge(tile):
    return min(tile, TILES - 1 - tile)


def last_tap(tile):
    return math.ceil(4 * MAXSHIFT * ((8 - edge(tile)) / TILES) ** 2) + TAPS - 1


def tap_count(tile):
    near, far = (7 - edge(tile)) / TILES, (8 - edge(tile)) / TILES
    return max(math.ceil(4 * s * far**2) - math.floor(4 * s * near**2) + 2 * TAPS - 1 for s in range(MAXSHIFT + 1))


def side_tiles(row):
    return sum(4 * MAXSHIFT * ((8 - e) / TILES) ** 2 > row - LOWER for e in range(TILES // 2))


COUNTS = [tap_count(t) for t in range(TILES)]
LASTS = [last_tap(t) for t in range(TILES)]
SIDES = [side_tiles(j) for j in range(UPPER)]
STARTS = [16 * sum(SIDES[:j]) for j in range(UPPER + 1)]


def from_behind(shard, axis, by):
    devices = lax.axis_size(axis)
    pairs = [(i, i + by) for i in range(devices) if 0 <= i + by < devices]
    return lax.ppermute(shard, axis, pairs)


def split(values):
    high = values.astype(jnp.bfloat16)
    low = (values - high.astype(jnp.float32)).astype(jnp.bfloat16)
    return high, low


def stack2(a, b, c, d):
    return jnp.concatenate([jnp.concatenate([a, b], axis=1), jnp.concatenate([c, d], axis=1)], axis=0)


def multiply(table, data, across):
    dims = (((1,), (1 if across else 0,)), ((), ()))

    def dot(x, y):
        return lax.dot_general(x, y, dims, preferred_element_type=jnp.float32)

    high, low = split(data)
    return dot(table[0][...], high) + (dot(table[0][...], low) + dot(table[1][...], high))


def quarters(values):
    n = FACTOR
    return values[:n, :n], values[:n, n:], values[n:, :n], values[n:, n:]


def transform_pair(re0, re1, im0, im1, first, twist, second, sign):
    a = multiply(first, stack2(re0, re1, im0, im1), False)
    r0, r1, i0, i1 = quarters(a)
    c, s = twist[0][...], twist[1][...]
    if sign < 0:
        turned = stack2(r0 * c + i0 * s, i0 * c - r0 * s, r1 * c + i1 * s, i1 * c - r1 * s)
    else:
        turned = stack2(r0 * c - i0 * s, i0 * c + r0 * s, r1 * c - i1 * s, i1 * c + r1 * s)
    return quarters(multiply(second, turned, True))


def fetcher(x, xs, sems):
    view = xs.reshape(FACTOR, PITCH, FACTOR)

    def fetch(g, part):
        rows = pl.ds(pl.multiple_of(8 * g, 8), 8)
        target = pl.ds(pl.multiple_of(32 * part + 8 * g, 8), 8)
        return pltpu.make_async_copy(x.at[:, part, rows, :], view.at[:, target, :], sems.at[g, part])

    return fetch


def forward_pair(xs, row, tables):
    def load(part, r):
        return xs[pl.ds(32 * part + r, FACTOR, stride=PITCH), :]

    return transform_pair(
        load(0, row), load(0, row + 1), load(1, row), load(1, row + 1), tables[0:2], tables[2:4], tables[4:6], -1
    )


def up_body(*refs):
    x, tables = refs[0], refs[1:7]
    up, xs, sems = refs[7:]
    fetch = fetcher(x, xs, sems)
    for g in (0, 1):
        for part in range(2):
            fetch(g, part).start()
    for row in range(0, UPPER, 2):
        if row % 8 == 0:
            for part in range(2):
                fetch(row // 8, part).wait()
        re0, re1, im0, im1 = forward_pair(xs, row, tables)
        for r, re, im in ((row, re0, im0), (row + 1, re1, im1)):
            if r < UPPER:
                start, size = STARTS[r], 8 * SIDES[r]
                for part, value in enumerate((re, im)):
                    up[part, start : start + size, :] = value[:size]
                    up[part, start + size : start + 2 * size, :] = value[FACTOR - size :]


def down_body(*refs):
    x, tables = refs[0], refs[1:7]
    _, down, xs, sems = refs[7:]
    fetch = fetcher(x, xs, sems)
    for part in range(2):
        fetch(3, part).start()
    for part in range(2):
        fetch(3, part).wait()
    for row in (28, 30):
        re0, re1, im0, im1 = forward_pair(xs, row, tables)
        for r, re, im in ((row, re0, im0), (row + 1, re1, im1)):
            if r >= 32 - LOWER:
                down[r - 32 + LOWER, 0] = re
                down[r - 32 + LOWER, 1] = im


def halo(body, shape, pairs, name, x, tables, after=None):
    first = [] if after is None else [after]
    return pl.pallas_call(
        body,
        in_specs=[pl.BlockSpec(memory_space=pl.ANY)]
        + [pl.BlockSpec(memory_space=pltpu.VMEM)] * 6
        + [pl.BlockSpec(memory_space=pl.ANY)] * len(first),
        out_shape=jax.ShapeDtypeStruct(shape, jnp.float32),
        scratch_shapes=[pltpu.VMEM((FACTOR * PITCH, FACTOR), jnp.float32), pltpu.SemaphoreType.DMA((4, 2))],
        compiler_params=pltpu.CompilerParams(vmem_limit_bytes=16 << 20),
        cost_estimate=pl.CostEstimate(flops=pairs << 29, bytes_accessed=pairs << 19, transcendentals=0),
        name=name,
    )(x, *tables, *first)


def up_rows(x, tables):
    return halo(up_body, (2, STARTS[-1], FACTOR), 8, "up", x, tables)


def down_rows(x, tables, after):
    return halo(down_body, (LOWER, 2) + PLANE, 2, "down", x, tables, after)


def arrange_body(x, out, stage, sems):
    parts, spans = x.shape[0], sems.shape[1]
    share = x.shape[1] // spans

    def take(i, part):
        span = pl.ds(i * share, share)
        return pltpu.make_async_copy(x.at[part, span], stage.at[span, part], sems.at[part, i])

    def give(i):
        span = pl.ds(i * share, share)
        return pltpu.make_async_copy(stage.at[span], out.at[span], sems.at[parts, i])

    for i in range(spans):
        for part in range(parts):
            take(i, part).start()
    for i in range(spans):
        for part in range(parts):
            take(i, part).wait()
        give(i).start()
    for i in range(spans):
        give(i).wait()


def arrange(blocks):
    parts, devices, rows, width = blocks.shape
    return pl.pallas_call(
        arrange_body,
        in_specs=[pl.BlockSpec(memory_space=pl.ANY)],
        out_specs=pl.BlockSpec(memory_space=pl.ANY),
        out_shape=jax.ShapeDtypeStruct((devices, parts, rows, width), jnp.float32),
        scratch_shapes=[
            pltpu.VMEM((devices, parts, rows, width), jnp.float32),
            pltpu.SemaphoreType.DMA((parts + 1, 8)),
        ],
        compiler_params=pltpu.CompilerParams(vmem_limit_bytes=60 << 20),
        cost_estimate=pl.CostEstimate(flops=1 << 20, bytes_accessed=8 << 20, transcendentals=0),
        name="arrange",
    )(blocks)


def forward_body(*refs):
    x, tables = refs[0], refs[1:7]
    spec, xs, sems = refs[7:]
    group = pl.program_id(0)
    fetch = fetcher(x, xs, sems)

    @pl.when(group == 0)
    def _():
        for g in range(4):
            for part in range(2):
                fetch(g, part).start()

    for part in range(2):
        fetch(group, part).wait()
    for local in range(0, 8, 2):
        re0, re1, im0, im1 = forward_pair(xs, 8 * group + local, tables)
        spec[local, 0] = re0
        spec[local + 1, 0] = re1
        spec[local, 1] = im0
        spec[local + 1, 1] = im1


def whole(shape):
    return pl.BlockSpec(shape, lambda *_: (0,) * len(shape))


def forward(x, tables):
    rows = x.shape[2]
    return pl.pallas_call(
        forward_body,
        grid=(rows // 8,),
        in_specs=[pl.BlockSpec(memory_space=pl.ANY)] + [whole(t.shape) for t in tables],
        out_specs=pl.BlockSpec((8, 2) + PLANE, lambda g: (g, 0, 0, 0)),
        out_shape=jax.ShapeDtypeStruct((rows, 2) + PLANE, jnp.float32),
        scratch_shapes=[pltpu.VMEM((FACTOR * PITCH, FACTOR), jnp.float32), pltpu.SemaphoreType.DMA((4, 2))],
        compiler_params=pltpu.CompilerParams(vmem_limit_bytes=16 << 20),
        cost_estimate=pl.CostEstimate(flops=8 << 30, bytes_accessed=8 << 20, transcendentals=0),
        name="forward",
    )(x, *tables)


def focus_rows(ext, taps, weights, chirp, tables, view, base, local):
    tiles = [[[], []] for _ in range(4)]
    for t in range(TILES):
        sub = slice(8 * t, 8 * t + 8)
        start = base + local + taps[t] + LOWER
        w = [weights[k, sub, :] for k in range(COUNTS[t])]
        sums = [[None, None] for _ in range(4)]
        for j in range(COUNTS[t] + 3):
            values = [ext[start + j, part, sub, :] for part in range(2)]
            for i in range(4):
                if 0 <= j - i < COUNTS[t]:
                    for part in range(2):
                        term = w[j - i] * values[part]
                        sums[i][part] = term if sums[i][part] is None else sums[i][part] + term
        for i in range(4):
            re, im = sums[i]
            c, s = chirp[local + i, 0, sub, :], chirp[local + i, 1, sub, :]
            tiles[i][0].append(re * c + im * s)
            tiles[i][1].append(im * c - re * s)
    planes = [[jnp.concatenate(part, axis=0) for part in row] for row in tiles]
    for i in (0, 2):
        (re0, im0), (re1, im1) = planes[i], planes[i + 1]
        re0, re1, im0, im1 = transform_pair(re0, re1, im0, im1, tables[0:2], tables[2:4], tables[4:6], 1)
        for part, r, value in ((0, 0, re0), (0, 1, re1), (1, 0, im0), (1, 1, im1)):
            view[pl.ds(FACTOR * 8 * part + local + i + r, FACTOR, stride=8), :] = value


def inner_body(*refs):
    taps, spec, down, weights, chirp = refs[:5]
    tables, (out, ext, sems) = refs[5:11], refs[11:]
    step = pl.program_id(0)
    count = 16 + UPPER

    @pl.when(step == 0)
    def _():
        copy = pltpu.make_async_copy(spec.at[pl.ds(0, count)], ext.at[pl.ds(LOWER, count)], sems.at[0])
        copy.start()
        for r in range(LOWER):
            ext[r] = down[r]
        copy.wait()

    view = out.reshape(2 * FACTOR * 8, FACTOR)
    for local in (0, 4):
        focus_rows(ext, taps, weights, chirp, tables, view, 8 * step, local)


def outer_body(*refs):
    taps, spec, up, weights, chirp = refs[:5]
    tables, (_, out, ext, sems) = refs[5:11], refs[11:]
    step = pl.program_id(0)
    rows = spec.shape[0]
    first = rows // 2 - LOWER

    @pl.when(step == 0)
    def _():
        count = rows - first
        copy = pltpu.make_async_copy(spec.at[pl.ds(first, count)], ext.at[pl.ds(first + LOWER, count)], sems.at[0])
        copy.start()
        for r in range(UPPER):
            start, size = STARTS[r], 8 * SIDES[r]
            for part in range(2):
                ext[LOWER + rows + r, part, :size, :] = up[part, start : start + size, :]
                ext[LOWER + rows + r, part, FACTOR - size :, :] = up[part, start + size : start + 2 * size, :]
        copy.wait()

    view = out.reshape(2 * FACTOR * 8, FACTOR)
    for local in (0, 4):
        focus_rows(ext, taps, weights, chirp, tables, view, rows // 2 + 8 * step, local)


def focus(group_of, steps, body, taps, operands, kinds, weights, chirp, tables, rows, prior, name):
    chunk = lambda g: (group_of(g), 0, 0, 0)
    image = pl.BlockSpec((2, None, FACTOR, 8, FACTOR), lambda g: (0, group_of(g), 0, 0, 0))
    specs = [pl.BlockSpec(memory_space=pltpu.SMEM)] + kinds + [whole(weights.shape), pl.BlockSpec((8, 2) + PLANE, chunk)]
    specs += [whole(t.shape) for t in tables]
    args = [taps, *operands, weights, chirp, *tables]
    aliases = {}
    if prior is not None:
        aliases = {len(args): 0}
        specs.append(pl.BlockSpec(memory_space=pl.ANY))
        args.append(prior)
    return pl.pallas_call(
        body,
        grid=(steps,),
        in_specs=specs,
        out_specs=image,
        out_shape=jax.ShapeDtypeStruct((2, rows // 8, FACTOR, 8, FACTOR), jnp.float32),
        input_output_aliases=aliases,
        scratch_shapes=[
            pltpu.VMEM((rows + LOWER + UPPER, 2) + PLANE, jnp.float32),
            pltpu.SemaphoreType.DMA((1,)),
        ],
        compiler_params=pltpu.CompilerParams(vmem_limit_bytes=24 << 20),
        cost_estimate=pl.CostEstimate(flops=steps * (3 << 30), bytes_accessed=steps * (4 << 20), transcendentals=0),
        name=name,
    )(*args)


def two_parts(values):
    high = lax.reduce_precision(values, 8, 7)
    return high.astype(jnp.bfloat16), (values - high).astype(jnp.bfloat16)


def turns(product, modulus):
    angle = 2.0 * math.pi / modulus * (product % modulus).astype(jnp.float32)
    return jnp.cos(angle), jnp.sin(angle)


def transform_tables(center, sign):
    start = (center - PULSES // 2) % PULSES
    index = jnp.arange(FACTOR, dtype=jnp.int32)
    fine, coarse = index + start % FACTOR, index + start // FACTOR

    def block(a, b):
        c, s = turns(a[:, None] * b[None, :], FACTOR)
        return two_parts(stack2(c, -sign * s, sign * s, c))

    if sign < 0:
        twist = turns(fine[:, None] * index[None, :], PULSES)
        return [*block(fine, index), *twist, *block(coarse, index)]
    twist = turns(index[:, None] * fine[None, :], PULSES)
    return [*block(index, coarse), *twist, *block(index, fine)]


def spectral_tables(distance, chirp_rate):
    index = jnp.arange(FACTOR, dtype=jnp.int32)
    bins = FACTOR * index[:, None] + index[None, :]
    relative = (bins - PULSES // 2).astype(jnp.float32) / PULSES
    migration = distance.astype(jnp.float32) * 4.0 * relative * relative
    nearness = jnp.array([(7 - edge(t)) ** 2 for t in range(TILES)], jnp.int32)
    latest = jnp.array([LASTS[t] - COUNTS[t] + 1 for t in range(TILES)], jnp.int32)
    taps = jnp.minimum(distance * nearness // (TILES * TILES // 4) - LOWER, latest)
    nearest = jnp.round(migration)
    sine = jnp.sin(math.pi * (migration - nearest)) / math.pi
    quarter = math.pi / TAPS
    offset = jnp.repeat(taps, 8)[None, :, None] + jnp.arange(max(COUNTS), dtype=jnp.int32)[:, None, None]
    away = offset.astype(jnp.float32) - migration
    sign = jnp.where((nearest.astype(jnp.int32) + offset) % 2 == 0, -1.0, 1.0)
    ratio = jnp.where(away == 0.0, 1.0, sign * sine / jnp.where(away == 0.0, 1.0, away))
    inside = jnp.abs(away) < TAPS
    weights = jnp.where(inside, ratio * (0.5 + 0.5 * jnp.cos(quarter * away)), 0.0)
    window = (0.54 + 0.46 * jnp.cos(2.0 * math.pi * relative)) / PULSES
    phase = math.pi * chirp_rate[:, None, None] * (relative * relative)
    return taps, weights, jnp.stack([window * jnp.cos(phase), window * jnp.sin(phase)], axis=1)


def compute(received, exchange, own, below, above, distance, chirp_rate):
    rows = received.shape[2]
    taps, weights, chirp = spectral_tables(distance, chirp_rate)
    inverse = transform_tables(own, 1)
    up = up_rows(received, transform_tables(below, -1))
    down = down_rows(received, transform_tables(above, -1), up)
    up, down = exchange(up, down)
    spec = forward(received, transform_tables(own, -1))
    anywhere = pl.BlockSpec(memory_space=pl.ANY)
    half = rows // 16
    shared = (weights, chirp, inverse, rows)
    image = focus(lambda g: g, half, inner_body, taps, [spec, down], [anywhere, whole(down.shape)], *shared, None, "inner")
    image = focus(lambda g: g + half, half, outer_body, taps, [spec, up], [anywhere, whole(up.shape)], *shared, image, "outer")
    return image.transpose(0, 1, 3, 2, 4).reshape(2, rows, PULSES)


def per_device(raw_echo, centroid, shifts, chirp_rate):
    devices = lax.axis_size("row")
    own_rows = raw_echo.shape[1] // devices
    blocks = raw_echo.reshape(2, devices, own_rows, raw_echo.shape[2])
    received = lax.all_to_all(arrange(blocks), "row", split_axis=0, concat_axis=0, tiled=True)

    def pick(values, device):
        block = jnp.clip(device, 0, devices - 1) * own_rows // BLOCK
        return jnp.sum(jnp.where(block == jnp.arange(values.shape[0], dtype=jnp.int32), values, 0))

    def exchange(up, down):
        return from_behind(up, "row", -1), from_behind(down, "row", 1)

    device = lax.axis_index("row")
    centers = [pick(centroid, device + by) for by in (0, -1, 1)]
    return compute(received, exchange, *centers, pick(shifts, device), chirp_rate)


def solution(mesh):
    return jax.shard_map(
        per_device,
        mesh=mesh,
        in_specs=(P(None, "slab", "row"), P("slab"), P("slab"), P(("slab", "row"))),
        out_specs=P(None, ("slab", "row"), None),
        check_vma=False,
    )
```

```python
import math

import jax
import jax.numpy as jnp
from jax import lax
from jax.experimental import pallas as pl
from jax.experimental.pallas import tpu as pltpu
from jax.sharding import PartitionSpec as P

FACTOR = 128
PULSES = 16384
BLOCK = 128
MAXSHIFT = 12
TAPS = 4
LOWER = TAPS - 1
UPPER = MAXSHIFT + TAPS - 1
PITCH = 72
TILES = FACTOR // 8
PLANE = (FACTOR, FACTOR)
DEPTH = FACTOR + 8
PADDED = (DEPTH, FACTOR)
TABLE = (2 * FACTOR, 2 * FACTOR)


def edge(tile):
    return min(tile, TILES - 1 - tile)


def last_tap(tile):
    return math.ceil(4 * MAXSHIFT * ((8 - edge(tile)) / TILES) ** 2) + TAPS - 1


def tap_count(tile):
    near, far = (7 - edge(tile)) / TILES, (8 - edge(tile)) / TILES
    return max(math.ceil(4 * s * far**2) - math.floor(4 * s * near**2) + 2 * TAPS - 1 for s in range(MAXSHIFT + 1))


def side_tiles(row):
    return sum(4 * MAXSHIFT * ((8 - e) / TILES) ** 2 > row - LOWER for e in range(TILES // 2))


COUNTS = [tap_count(t) for t in range(TILES)]
LASTS = [last_tap(t) for t in range(TILES)]
SIDES = [side_tiles(j) for j in range(UPPER)]
STARTS = [16 * sum(SIDES[:j]) for j in range(UPPER + 1)]


def from_behind(shard, axis, by):
    devices = lax.axis_size(axis)
    pairs = [(i, i + by) for i in range(devices) if 0 <= i + by < devices]
    return lax.ppermute(shard, axis, pairs)


def split(values):
    high = values.astype(jnp.bfloat16)
    low = (values - high.astype(jnp.float32)).astype(jnp.bfloat16)
    return high, low


def stack2(a, b, c, d):
    return jnp.concatenate([jnp.concatenate([a, b], axis=1), jnp.concatenate([c, d], axis=1)], axis=0)


def multiply(table, data, across):
    dims = (((1,), (1 if across else 0,)), ((), ()))

    def dot(x, y):
        return lax.dot_general(x, y, dims, preferred_element_type=jnp.float32)

    high, low = split(data)
    half = 2 * FACTOR
    both = dot(table[...], high)
    return both[:half] + dot(table[:half, :], low) + both[half:]


def quarters(values):
    n = FACTOR
    return values[:n, :n], values[:n, n:], values[n:, :n], values[n:, n:]


def transform_pairs(pairs, first, twist, second, sign):
    middle = [multiply(first, stack2(*pair), False) for pair in pairs]
    c, s = twist[0][...], twist[1][...]
    turned = []
    for a in middle:
        r0, r1, i0, i1 = quarters(a)
        if sign < 0:
            turned.append(stack2(r0 * c + i0 * s, i0 * c - r0 * s, r1 * c + i1 * s, i1 * c - r1 * s))
        else:
            turned.append(stack2(r0 * c - i0 * s, i0 * c + r0 * s, r1 * c - i1 * s, i1 * c + r1 * s))
    return [quarters(multiply(second, t, True)) for t in turned]


def fetcher(x, xs, sems):
    view = xs.reshape(FACTOR, PITCH, FACTOR)

    def fetch(g, part):
        rows = pl.ds(pl.multiple_of(8 * g, 8), 8)
        target = pl.ds(pl.multiple_of(32 * part + 8 * g, 8), 8)
        return pltpu.make_async_copy(x.at[:, part, rows, :], view.at[:, target, :], sems.at[g, part])

    return fetch


def forward_rows(xs, rows, tables):
    def load(part, r):
        return xs[pl.ds(32 * part + r, FACTOR, stride=PITCH), :]

    pairs = [(load(0, row), load(0, row + 1), load(1, row), load(1, row + 1)) for row in rows]
    results = transform_pairs(pairs, tables[0], tables[1:3], tables[3], -1)
    for row, (re0, re1, im0, im1) in zip(rows, results):
        yield row, re0, im0
        yield row + 1, re1, im1


def halo_body(*refs):
    x, up_tables, down_tables = refs[0], refs[1:5], refs[5:9]
    up, down, xs, sems = refs[9:]
    fetch = fetcher(x, xs, sems)
    for g in (0, 1, 3):
        for part in range(2):
            fetch(g, part).start()
    for first in range(0, UPPER, 4):
        if first % 8 == 0:
            for part in range(2):
                fetch(first // 8, part).wait()
        for r, re, im in forward_rows(xs, (first, first + 2), up_tables):
            if r < UPPER:
                start, size = STARTS[r], 8 * SIDES[r]
                for part, value in enumerate((re, im)):
                    up[part, start : start + size, :] = value[:size]
                    up[part, start + size : start + 2 * size, :] = value[FACTOR - size :]
    for part in range(2):
        fetch(3, part).wait()
    for r, re, im in forward_rows(xs, (28, 30), down_tables):
        if r >= 32 - LOWER:
            down[r - 32 + LOWER, 0] = re
            down[r - 32 + LOWER, 1] = im


def halo(x, up_tables, down_tables):
    shapes = [(2, STARTS[-1], FACTOR), (LOWER, 2) + PLANE]
    return pl.pallas_call(
        halo_body,
        in_specs=[pl.BlockSpec(memory_space=pl.ANY)] + [pl.BlockSpec(memory_space=pltpu.VMEM)] * 8,
        out_shape=[jax.ShapeDtypeStruct(shape, jnp.float32) for shape in shapes],
        scratch_shapes=[pltpu.VMEM((FACTOR * PITCH, FACTOR), jnp.float32), pltpu.SemaphoreType.DMA((4, 2))],
        compiler_params=pltpu.CompilerParams(vmem_limit_bytes=16 << 20),
        cost_estimate=pl.CostEstimate(flops=5 << 30, bytes_accessed=5 << 20, transcendentals=0),
        name="halo",
    )(x, *up_tables, *down_tables)


def arrange_body(x, out, stage, sems):
    parts, spans = x.shape[0], sems.shape[1]
    share = x.shape[1] // spans

    def take(i, part):
        span = pl.ds(i * share, share)
        return pltpu.make_async_copy(x.at[part, span], stage.at[span, part], sems.at[part, i])

    def give(i):
        span = pl.ds(i * share, share)
        return pltpu.make_async_copy(stage.at[span], out.at[span], sems.at[parts, i])

    for i in range(spans):
        for part in range(parts):
            take(i, part).start()
    for i in range(spans):
        for part in range(parts):
            take(i, part).wait()
        give(i).start()
    for i in range(spans):
        give(i).wait()


def arrange(blocks):
    parts, devices, rows, width = blocks.shape
    return pl.pallas_call(
        arrange_body,
        in_specs=[pl.BlockSpec(memory_space=pl.ANY)],
        out_specs=pl.BlockSpec(memory_space=pl.ANY),
        out_shape=jax.ShapeDtypeStruct((devices, parts, rows, width), jnp.float32),
        scratch_shapes=[
            pltpu.VMEM((devices, parts, rows, width), jnp.float32),
            pltpu.SemaphoreType.DMA((parts + 1, 8)),
        ],
        compiler_params=pltpu.CompilerParams(vmem_limit_bytes=60 << 20),
        cost_estimate=pl.CostEstimate(flops=1 << 20, bytes_accessed=8 << 20, transcendentals=0),
        name="arrange",
    )(blocks)


def forward_body(*refs):
    x, tables = refs[0], refs[1:5]
    spec, xs, sems = refs[5:]
    group = pl.program_id(0)
    fetch = fetcher(x, xs, sems)

    @pl.when(group == 0)
    def _():
        for g in range(4):
            for part in range(2):
                fetch(g, part).start()

    for part in range(2):
        fetch(group, part).wait()
    for local in (0, 4):
        rows = (8 * group + local, 8 * group + local + 2)
        for i, (_, re, im) in enumerate(forward_rows(xs, rows, tables)):
            spec[local + i, 0, :FACTOR, :] = re
            spec[local + i, 1, :FACTOR, :] = im


def whole(shape):
    return pl.BlockSpec(shape, lambda *_: (0,) * len(shape))


def forward(x, tables):
    rows = x.shape[2]
    return pl.pallas_call(
        forward_body,
        grid=(rows // 8,),
        in_specs=[pl.BlockSpec(memory_space=pl.ANY)] + [whole(t.shape) for t in tables],
        out_specs=pl.BlockSpec((8, 2) + PADDED, lambda g: (g, 0, 0, 0)),
        out_shape=jax.ShapeDtypeStruct((rows, 2) + PADDED, jnp.float32),
        scratch_shapes=[pltpu.VMEM((FACTOR * PITCH, FACTOR), jnp.float32), pltpu.SemaphoreType.DMA((4, 2))],
        compiler_params=pltpu.CompilerParams(vmem_limit_bytes=16 << 20),
        cost_estimate=pl.CostEstimate(flops=8 << 30, bytes_accessed=8 << 20, transcendentals=0),
        name="forward",
    )(x, *tables)


def focus_rows(source, shift, taps, weights, chirp, tables, view, first, slot):
    tiles = [[[], []] for _ in range(4)]
    for t in range(TILES):
        sub = slice(8 * t, 8 * t + 8)
        start = first + taps[t] + shift
        w = [weights[k, sub, :] for k in range(COUNTS[t])]
        sums = [[None, None] for _ in range(4)]
        for j in range(COUNTS[t] + 3):
            values = [source[start + j, part, sub, :] for part in range(2)]
            for i in range(4):
                if 0 <= j - i < COUNTS[t]:
                    for part in range(2):
                        term = w[j - i] * values[part]
                        sums[i][part] = term if sums[i][part] is None else sums[i][part] + term
        for i in range(4):
            re, im = sums[i]
            c, s = chirp[first + i, 0, sub, :], chirp[first + i, 1, sub, :]
            tiles[i][0].append(re * c + im * s)
            tiles[i][1].append(im * c - re * s)
    planes = [[jnp.concatenate(part, axis=0) for part in row] for row in tiles]
    pairs = [(planes[i][0], planes[i + 1][0], planes[i][1], planes[i + 1][1]) for i in (0, 2)]
    results = transform_pairs(pairs, tables[0], tables[1:3], tables[3], 1)
    for i, (re0, re1, im0, im1) in zip((0, 2), results):
        for part, r, value in ((0, 0, re0), (0, 1, re1), (1, 0, im0), (1, 1, im1)):
            view[pl.ds(FACTOR * 8 * part + slot + i + r, FACTOR, stride=8), :] = value


GROUP = 2 * FACTOR * 8


def inner_body(*refs):
    taps, spec, down, weights, chirp = refs[:5]
    tables, (out, ext, image, sems) = refs[5:9], refs[9:]
    count = 4 + UPPER
    copy = pltpu.make_async_copy(spec.at[pl.ds(0, count)], ext.at[pl.ds(LOWER, count)], sems.at[0])
    copy.start()
    view = image.reshape(2 * GROUP, FACTOR)
    gives = [pltpu.make_async_copy(image.at[g], out.at[:, g], sems.at[1 + g]) for g in range(2)]

    def quad(k, carry):
        slot = (k // 2) * GROUP + 4 * (k % 2)
        focus_rows(spec, 0, taps, weights, chirp, tables, view, 4 * k, slot)
        return carry

    quad(2, 0)
    quad(3, 0)
    gives[1].start()
    for r in range(LOWER):
        ext[r, :, :FACTOR, :] = down[r]
    copy.wait()
    quad(1, 0)
    focus_rows(ext, LOWER, taps, weights, chirp, tables, view, 0, 0)
    gives[0].start()
    for give in gives:
        give.wait()


def outer_body(*refs):
    taps, spec, up, weights, chirp = refs[:5]
    tables, (_, out, ext, image, sems) = refs[5:9], refs[9:]
    rows = spec.shape[0]
    half = rows // 2
    below = half - LOWER
    copy = pltpu.make_async_copy(spec.at[pl.ds(below, rows - below)], ext.at[pl.ds(0, rows - below)], sems.at[0])
    copy.start()
    for r in range(UPPER):
        start, size = STARTS[r], 8 * SIDES[r]
        for part in range(2):
            ext[rows - below + r, part, :size, :] = up[part, start : start + size, :]
            ext[rows - below + r, part, FACTOR - size : FACTOR, :] = up[part, start + size : start + 2 * size, :]
    copy.wait()
    view = image.reshape(2 * GROUP, FACTOR)

    def give(g):
        return pltpu.make_async_copy(image.at[g], out.at[:, half // 8 + g], sems.at[1 + g])

    def group(g, carry):
        for local in (0, 4):
            focus_rows(ext, -below, taps, weights, chirp, tables, view, half + 8 * g + local, GROUP * g + local)
        give(g).start()
        return carry

    lax.fori_loop(0, 2, group, 0)
    for g in range(2):
        give(g).wait()


def focus(body, depth, taps, operands, weights, chirp, tables, rows, prior, name):
    inside, anywhere = pl.BlockSpec(memory_space=pltpu.VMEM), pl.BlockSpec(memory_space=pl.ANY)
    args = [taps, *operands, weights, chirp, *tables]
    specs = [pl.BlockSpec(memory_space=pltpu.SMEM)] + [inside] * (len(args) - 1)
    aliases = {}
    if prior is not None:
        aliases = {len(args): 0}
        specs.append(anywhere)
        args.append(prior)
    return pl.pallas_call(
        body,
        in_specs=specs,
        out_specs=anywhere,
        out_shape=jax.ShapeDtypeStruct((2, rows // 8, FACTOR, 8, FACTOR), jnp.float32),
        input_output_aliases=aliases,
        scratch_shapes=[
            pltpu.VMEM((depth, 2) + PADDED, jnp.float32),
            pltpu.VMEM((2, 2, FACTOR, 8, FACTOR), jnp.float32),
            pltpu.SemaphoreType.DMA((3,)),
        ],
        compiler_params=pltpu.CompilerParams(vmem_limit_bytes=26 << 20),
        cost_estimate=pl.CostEstimate(flops=6 << 30, bytes_accessed=8 << 20, transcendentals=0),
        name=name,
    )(*args)


def two_parts(values):
    high = lax.reduce_precision(values, 8, 7)
    return jnp.concatenate([high.astype(jnp.bfloat16), (values - high).astype(jnp.bfloat16)])


def turns(product, modulus):
    angle = 2.0 * math.pi / modulus * (product % modulus).astype(jnp.float32)
    return jnp.cos(angle), jnp.sin(angle)


def transform_tables(center, sign):
    start = (center - PULSES // 2) % PULSES
    index = jnp.arange(FACTOR, dtype=jnp.int32)
    fine, coarse = index + start % FACTOR, index + start // FACTOR

    def block(a, b):
        c, s = turns(a[:, None] * b[None, :], FACTOR)
        return two_parts(stack2(c, -sign * s, sign * s, c))

    if sign < 0:
        twist = turns(fine[:, None] * index[None, :], PULSES)
        return [block(fine, index), *twist, block(coarse, index)]
    twist = turns(index[:, None] * fine[None, :], PULSES)
    return [block(index, coarse), *twist, block(index, fine)]


def spectral_tables(distance, chirp_rate):
    index = jnp.arange(FACTOR, dtype=jnp.int32)
    bins = FACTOR * index[:, None] + index[None, :]
    relative = (bins - PULSES // 2).astype(jnp.float32) / PULSES
    migration = distance.astype(jnp.float32) * 4.0 * relative * relative
    nearness = jnp.array([(7 - edge(t)) ** 2 for t in range(TILES)], jnp.int32)
    latest = jnp.array([LASTS[t] - COUNTS[t] + 1 for t in range(TILES)], jnp.int32)
    taps = jnp.minimum(distance * nearness // (TILES * TILES // 4) - LOWER, latest)
    nearest = jnp.round(migration)
    sine = jnp.sin(math.pi * (migration - nearest)) / math.pi
    quarter = math.pi / TAPS
    offset = jnp.repeat(taps, 8)[None, :, None] + jnp.arange(max(COUNTS), dtype=jnp.int32)[:, None, None]
    away = offset.astype(jnp.float32) - migration
    sign = jnp.where((nearest.astype(jnp.int32) + offset) % 2 == 0, -1.0, 1.0)
    ratio = jnp.where(away == 0.0, 1.0, sign * sine / jnp.where(away == 0.0, 1.0, away))
    inside = jnp.abs(away) < TAPS
    weights = jnp.where(inside, ratio * (0.5 + 0.5 * jnp.cos(quarter * away)), 0.0)
    window = (0.54 + 0.46 * jnp.cos(2.0 * math.pi * relative)) / PULSES
    phase = math.pi * chirp_rate[:, None, None] * (relative * relative)
    weights = jnp.pad(weights, ((0, 0), (0, DEPTH - FACTOR), (0, 0)))
    return taps, weights, jnp.stack([window * jnp.cos(phase), window * jnp.sin(phase)], axis=1)


def compute(received, exchange, own, below, above, distance, chirp_rate):
    rows = received.shape[2]
    taps, weights, chirp = spectral_tables(distance, chirp_rate)
    inverse = transform_tables(own, 1)
    up, down = exchange(*halo(received, transform_tables(below, -1), transform_tables(above, -1)))
    spec = forward(received, transform_tables(own, -1))
    shared = (weights, chirp, inverse, rows)
    image = focus(inner_body, LOWER + 4 + UPPER, taps, [spec, down], *shared, None, "inner")
    image = focus(outer_body, LOWER + rows // 2 + UPPER, taps, [spec, up], *shared, image, "outer")
    return image.transpose(0, 1, 3, 2, 4).reshape(2, rows, PULSES)


def per_device(raw_echo, centroid, shifts, chirp_rate):
    devices = lax.axis_size("row")
    own_rows = raw_echo.shape[1] // devices
    blocks = raw_echo.reshape(2, devices, own_rows, raw_echo.shape[2])
    received = lax.all_to_all(arrange(blocks), "row", split_axis=0, concat_axis=0, tiled=True)

    def pick(values, device):
        block = jnp.clip(device, 0, devices - 1) * own_rows // BLOCK
        return jnp.sum(jnp.where(block == jnp.arange(values.shape[0], dtype=jnp.int32), values, 0))

    def exchange(up, down):
        return from_behind(up, "row", -1), from_behind(down, "row", 1)

    device = lax.axis_index("row")
    centers = [pick(centroid, device + by) for by in (0, -1, 1)]
    return compute(received, exchange, *centers, pick(shifts, device), chirp_rate)


def solution(mesh):
    return jax.shard_map(
        per_device,
        mesh=mesh,
        in_specs=(P(None, "slab", "row"), P("slab"), P("slab"), P(("slab", "row"))),
        out_specs=P(None, ("slab", "row"), None),
        check_vma=False,
    )
```

```python
import math

import jax
import jax.numpy as jnp
from jax import lax
from jax.experimental import pallas as pl
from jax.experimental.pallas import tpu as pltpu
from jax.sharding import PartitionSpec as P

FACTOR = 128
PULSES = 16384
BLOCK = 128
MAXSHIFT = 12
TAPS = 4
LOWER = TAPS - 1
UPPER = MAXSHIFT + TAPS - 1
PITCH = 72
TILES = FACTOR // 8
PLANE = (FACTOR, FACTOR)
DEPTH = FACTOR + 8
PADDED = (DEPTH, FACTOR)


def edge(tile):
    return min(tile, TILES - 1 - tile)


def last_tap(tile):
    return math.ceil(4 * MAXSHIFT * ((8 - edge(tile)) / TILES) ** 2) + TAPS - 1


def tap_count(tile):
    near, far = (7 - edge(tile)) / TILES, (8 - edge(tile)) / TILES
    return max(math.ceil(4 * s * far**2) - math.floor(4 * s * near**2) + 2 * TAPS - 1 for s in range(MAXSHIFT + 1))


def side_tiles(row):
    return sum(4 * MAXSHIFT * ((8 - e) / TILES) ** 2 > row - LOWER for e in range(TILES // 2))


COUNTS = [tap_count(t) for t in range(TILES)]
LASTS = [last_tap(t) for t in range(TILES)]
SIDES = [side_tiles(j) for j in range(UPPER)]
STARTS = [16 * sum(SIDES[:j]) for j in range(UPPER + 1)]


def from_behind(shard, axis, by):
    devices = lax.axis_size(axis)
    pairs = [(i, i + by) for i in range(devices) if 0 <= i + by < devices]
    return lax.ppermute(shard, axis, pairs)


def split(values):
    high = values.astype(jnp.bfloat16)
    low = (values - high.astype(jnp.float32)).astype(jnp.bfloat16)
    return high, low


def stack2(a, b, c, d):
    return jnp.concatenate([jnp.concatenate([a, b], axis=1), jnp.concatenate([c, d], axis=1)], axis=0)


def multiply(table, data, across):
    dims = (((1,), (1 if across else 0,)), ((), ()))

    def dot(x, y):
        return lax.dot_general(x, y, dims, preferred_element_type=jnp.float32)

    high, low = split(data)
    half = 2 * FACTOR
    both = dot(table[...], high)
    return both[:half] + dot(table[:half, :], low) + both[half:]


def quarters(values):
    n = FACTOR
    return values[:n, :n], values[:n, n:], values[n:, :n], values[n:, n:]


def transform_pairs(pairs, first, twist, second, sign):
    middle = [multiply(first, stack2(*pair), False) for pair in pairs]
    c, s = twist[0][...], twist[1][...]
    turned = []
    for a in middle:
        r0, r1, i0, i1 = quarters(a)
        if sign < 0:
            turned.append(stack2(r0 * c + i0 * s, i0 * c - r0 * s, r1 * c + i1 * s, i1 * c - r1 * s))
        else:
            turned.append(stack2(r0 * c - i0 * s, i0 * c + r0 * s, r1 * c - i1 * s, i1 * c + r1 * s))
    return [quarters(multiply(second, t, True)) for t in turned]


def fetcher(x, xs, sems):
    view = xs.reshape(FACTOR, PITCH, FACTOR)

    def fetch(g, part):
        rows = pl.ds(pl.multiple_of(8 * g, 8), 8)
        target = pl.ds(pl.multiple_of(32 * part + 8 * g, 8), 8)
        return pltpu.make_async_copy(x.at[:, part, rows, :], view.at[:, target, :], sems.at[g, part])

    return fetch


def forward_rows(xs, rows, tables):
    def load(part, r):
        return xs[pl.ds(32 * part + r, FACTOR, stride=PITCH), :]

    pairs = [(load(0, row), load(0, row + 1), load(1, row), load(1, row + 1)) for row in rows]
    results = transform_pairs(pairs, tables[0], tables[1:3], tables[3], -1)
    for row, (re0, re1, im0, im1) in zip(rows, results):
        yield row, re0, im0
        yield row + 1, re1, im1


def halo_body(*refs):
    x, up_tables, down_tables = refs[0], refs[1:5], refs[5:9]
    up, down, xs, sems = refs[9:]
    fetch = fetcher(x, xs, sems)
    for g in (0, 1, 3):
        for part in range(2):
            fetch(g, part).start()
    for first in range(0, UPPER, 4):
        if first % 8 == 0:
            for part in range(2):
                fetch(first // 8, part).wait()
        for r, re, im in forward_rows(xs, (first, first + 2), up_tables):
            if r < UPPER:
                start, size = STARTS[r], 8 * SIDES[r]
                for part, value in enumerate((re, im)):
                    up[part, start : start + size, :] = value[:size]
                    up[part, start + size : start + 2 * size, :] = value[FACTOR - size :]
    for part in range(2):
        fetch(3, part).wait()
    for r, re, im in forward_rows(xs, (28, 30), down_tables):
        if r >= 32 - LOWER:
            down[r - 32 + LOWER, 0] = re
            down[r - 32 + LOWER, 1] = im


def halo(x, up_tables, down_tables):
    shapes = [(2, STARTS[-1], FACTOR), (LOWER, 2) + PLANE]
    return pl.pallas_call(
        halo_body,
        in_specs=[pl.BlockSpec(memory_space=pl.ANY)] + [pl.BlockSpec(memory_space=pltpu.VMEM)] * 8,
        out_shape=[jax.ShapeDtypeStruct(shape, jnp.float32) for shape in shapes],
        scratch_shapes=[pltpu.VMEM((FACTOR * PITCH, FACTOR), jnp.float32), pltpu.SemaphoreType.DMA((4, 2))],
        compiler_params=pltpu.CompilerParams(vmem_limit_bytes=16 << 20),
        cost_estimate=pl.CostEstimate(flops=5 << 30, bytes_accessed=5 << 20, transcendentals=0),
        name="halo",
    )(x, *up_tables, *down_tables)


def arrange_body(x, out, stage, sems):
    parts, spans = x.shape[0], sems.shape[1]
    share = x.shape[1] // spans

    def take(i, part):
        span = pl.ds(i * share, share)
        return pltpu.make_async_copy(x.at[part, span], stage.at[span, part], sems.at[part, i])

    def give(i):
        span = pl.ds(i * share, share)
        return pltpu.make_async_copy(stage.at[span], out.at[span], sems.at[parts, i])

    for i in range(spans):
        for part in range(parts):
            take(i, part).start()
    for i in range(spans):
        for part in range(parts):
            take(i, part).wait()
        give(i).start()
    for i in range(spans):
        give(i).wait()


def arrange(blocks):
    parts, devices, rows, width = blocks.shape
    return pl.pallas_call(
        arrange_body,
        in_specs=[pl.BlockSpec(memory_space=pl.ANY)],
        out_specs=pl.BlockSpec(memory_space=pl.ANY),
        out_shape=jax.ShapeDtypeStruct((devices, parts, rows, width), jnp.float32),
        scratch_shapes=[
            pltpu.VMEM((devices, parts, rows, width), jnp.float32),
            pltpu.SemaphoreType.DMA((parts + 1, 8)),
        ],
        compiler_params=pltpu.CompilerParams(vmem_limit_bytes=60 << 20),
        cost_estimate=pl.CostEstimate(flops=1 << 20, bytes_accessed=8 << 20, transcendentals=0),
        name="arrange",
    )(blocks)


def forward_body(*refs):
    x, tables = refs[0], refs[1:5]
    spec, xs, sems = refs[5:]
    group = pl.program_id(0)
    fetch = fetcher(x, xs, sems)

    @pl.when(group == 0)
    def _():
        for g in range(4):
            for part in range(2):
                fetch(g, part).start()

    for part in range(2):
        fetch(group, part).wait()
    for local in (0, 4):
        rows = (8 * group + local, 8 * group + local + 2)
        for i, (_, re, im) in enumerate(forward_rows(xs, rows, tables)):
            spec[local + i, 0, :FACTOR, :] = re
            spec[local + i, 1, :FACTOR, :] = im


def whole(shape):
    return pl.BlockSpec(shape, lambda *_: (0,) * len(shape))


def forward(x, tables):
    rows = x.shape[2]
    return pl.pallas_call(
        forward_body,
        grid=(rows // 8,),
        in_specs=[pl.BlockSpec(memory_space=pl.ANY)] + [whole(t.shape) for t in tables],
        out_specs=pl.BlockSpec((8, 2) + PADDED, lambda g: (g, 0, 0, 0)),
        out_shape=jax.ShapeDtypeStruct((rows, 2) + PADDED, jnp.float32),
        scratch_shapes=[pltpu.VMEM((FACTOR * PITCH, FACTOR), jnp.float32), pltpu.SemaphoreType.DMA((4, 2))],
        compiler_params=pltpu.CompilerParams(vmem_limit_bytes=16 << 20),
        cost_estimate=pl.CostEstimate(flops=8 << 30, bytes_accessed=8 << 20, transcendentals=0),
        name="forward",
    )(x, *tables)


def focus_rows(source, shift, taps, weights, chirp, tables, view, first, slot):
    tiles = [[[], []] for _ in range(4)]
    for t in range(TILES):
        sub = slice(8 * t, 8 * t + 8)
        start = first + taps[t] + shift
        w = [weights[k, sub, :] for k in range(COUNTS[t])]
        sums = [[None, None] for _ in range(4)]
        for j in range(COUNTS[t] + 3):
            values = [source[start + j, part, sub, :] for part in range(2)]
            for i in range(4):
                if 0 <= j - i < COUNTS[t]:
                    for part in range(2):
                        term = w[j - i] * values[part]
                        sums[i][part] = term if sums[i][part] is None else sums[i][part] + term
        for i in range(4):
            re, im = sums[i]
            c, s = chirp[first + i, 0, sub, :], chirp[first + i, 1, sub, :]
            tiles[i][0].append(re * c + im * s)
            tiles[i][1].append(im * c - re * s)
    planes = [[jnp.concatenate(part, axis=0) for part in row] for row in tiles]
    pairs = [(planes[i][0], planes[i + 1][0], planes[i][1], planes[i + 1][1]) for i in (0, 2)]
    results = transform_pairs(pairs, tables[0], tables[1:3], tables[3], 1)
    for i, (re0, re1, im0, im1) in zip((0, 2), results):
        for part, r, value in ((0, 0, re0), (0, 1, re1), (1, 0, im0), (1, 1, im1)):
            view[pl.ds(FACTOR * 8 * part + slot + i + r, FACTOR, stride=8), :] = value


GROUP = 2 * FACTOR * 8


def inner_body(*refs):
    taps, spec, down, weights, chirp = refs[:5]
    tables, (out, ext, image, sems) = refs[5:9], refs[9:]
    count = 4 + UPPER
    copy = pltpu.make_async_copy(spec.at[pl.ds(0, count)], ext.at[pl.ds(LOWER, count)], sems.at[0])
    copy.start()
    view = image.reshape(2 * GROUP, FACTOR)
    gives = [pltpu.make_async_copy(image.at[g], out.at[:, g], sems.at[1 + g]) for g in range(2)]

    def quad(k, carry):
        slot = (k // 2) * GROUP + 4 * (k % 2)
        focus_rows(spec, 0, taps, weights, chirp, tables, view, 4 * k, slot)
        return carry

    quad(2, 0)
    quad(3, 0)
    gives[1].start()
    for r in range(LOWER):
        ext[r, :, :FACTOR, :] = down[r]
    copy.wait()
    quad(1, 0)
    focus_rows(ext, LOWER, taps, weights, chirp, tables, view, 0, 0)
    gives[0].start()
    for give in gives:
        give.wait()


def outer_body(*refs):
    taps, spec, up, weights, chirp = refs[:5]
    tables, (_, out, ext, image, sems) = refs[5:9], refs[9:]
    rows = spec.shape[0]
    half = rows // 2
    below = half - LOWER
    copy = pltpu.make_async_copy(spec.at[pl.ds(below, rows - below)], ext.at[pl.ds(0, rows - below)], sems.at[0])
    copy.start()
    for r in range(UPPER):
        start, size = STARTS[r], 8 * SIDES[r]
        for part in range(2):
            ext[rows - below + r, part, :size, :] = up[part, start : start + size, :]
            ext[rows - below + r, part, FACTOR - size : FACTOR, :] = up[part, start + size : start + 2 * size, :]
    copy.wait()
    view = image.reshape(2 * GROUP, FACTOR)

    def give(g):
        return pltpu.make_async_copy(image.at[g], out.at[:, half // 8 + g], sems.at[1 + g])

    def group(g, carry):
        for local in (0, 4):
            focus_rows(ext, -below, taps, weights, chirp, tables, view, half + 8 * g + local, GROUP * g + local)
        give(g).start()
        return carry

    lax.fori_loop(0, 2, group, 0)
    for g in range(2):
        give(g).wait()


def focus(body, depth, taps, operands, weights, chirp, tables, rows, prior):
    inside, anywhere = pl.BlockSpec(memory_space=pltpu.VMEM), pl.BlockSpec(memory_space=pl.ANY)
    args = [taps, *operands, weights, chirp, *tables]
    specs = [pl.BlockSpec(memory_space=pltpu.SMEM)] + [inside] * (len(args) - 1)
    aliases = {}
    if prior is not None:
        aliases = {len(args): 0}
        specs.append(anywhere)
        args.append(prior)
    return pl.pallas_call(
        body,
        in_specs=specs,
        out_specs=anywhere,
        out_shape=jax.ShapeDtypeStruct((2, rows // 8, FACTOR, 8, FACTOR), jnp.float32),
        input_output_aliases=aliases,
        scratch_shapes=[
            pltpu.VMEM((depth, 2) + PADDED, jnp.float32),
            pltpu.VMEM((2, 2, FACTOR, 8, FACTOR), jnp.float32),
            pltpu.SemaphoreType.DMA((3,)),
        ],
        compiler_params=pltpu.CompilerParams(vmem_limit_bytes=26 << 20),
        cost_estimate=pl.CostEstimate(flops=6 << 30, bytes_accessed=8 << 20, transcendentals=0),
    )(*args)


def two_parts(values):
    high = lax.reduce_precision(values, 8, 7)
    return jnp.concatenate([high.astype(jnp.bfloat16), (values - high).astype(jnp.bfloat16)])


def turns(product, modulus):
    angle = 2.0 * math.pi / modulus * (product % modulus).astype(jnp.float32)
    return jnp.cos(angle), jnp.sin(angle)


def transform_tables(center, sign):
    start = (center - PULSES // 2) % PULSES
    index = jnp.arange(FACTOR, dtype=jnp.int32)
    fine, coarse = index + start % FACTOR, index + start // FACTOR

    def block(a, b):
        c, s = turns(a[:, None] * b[None, :], FACTOR)
        return two_parts(stack2(c, -sign * s, sign * s, c))

    if sign < 0:
        twist = turns(fine[:, None] * index[None, :], PULSES)
        return [block(fine, index), *twist, block(coarse, index)]
    twist = turns(index[:, None] * fine[None, :], PULSES)
    return [block(index, coarse), *twist, block(index, fine)]


def spectral_tables(distance, chirp_rate):
    index = jnp.arange(FACTOR, dtype=jnp.int32)
    bins = FACTOR * index[:, None] + index[None, :]
    relative = (bins - PULSES // 2).astype(jnp.float32) / PULSES
    migration = distance.astype(jnp.float32) * 4.0 * relative * relative
    nearness = jnp.array([(7 - edge(t)) ** 2 for t in range(TILES)], jnp.int32)
    latest = jnp.array([LASTS[t] - COUNTS[t] + 1 for t in range(TILES)], jnp.int32)
    taps = jnp.minimum(distance * nearness // (TILES * TILES // 4) - LOWER, latest)
    nearest = jnp.round(migration)
    sine = jnp.sin(math.pi * (migration - nearest)) / math.pi
    quarter = math.pi / TAPS
    offset = jnp.repeat(taps, 8)[None, :, None] + jnp.arange(max(COUNTS), dtype=jnp.int32)[:, None, None]
    away = offset.astype(jnp.float32) - migration
    sign = jnp.where((nearest.astype(jnp.int32) + offset) % 2 == 0, -1.0, 1.0)
    ratio = jnp.where(away == 0.0, 1.0, sign * sine / jnp.where(away == 0.0, 1.0, away))
    inside = jnp.abs(away) < TAPS
    weights = jnp.where(inside, ratio * (0.5 + 0.5 * jnp.cos(quarter * away)), 0.0)
    window = (0.54 + 0.46 * jnp.cos(2.0 * math.pi * relative)) / PULSES
    phase = math.pi * chirp_rate[:, None, None] * (relative * relative)
    weights = jnp.pad(weights, ((0, 0), (0, DEPTH - FACTOR), (0, 0)))
    return taps, weights, jnp.stack([window * jnp.cos(phase), window * jnp.sin(phase)], axis=1)


def compute(received, exchange, own, below, above, distance, chirp_rate):
    rows = received.shape[2]
    taps, weights, chirp = spectral_tables(distance, chirp_rate)
    inverse = transform_tables(own, 1)
    up, down = exchange(*halo(received, transform_tables(below, -1), transform_tables(above, -1)))
    spec = forward(received, transform_tables(own, -1))
    shared = (weights, chirp, inverse, rows)
    image = focus(inner_body, LOWER + 4 + UPPER, taps, [spec, down], *shared, None)
    image = focus(outer_body, LOWER + rows // 2 + UPPER, taps, [spec, up], *shared, image)
    return image.transpose(0, 1, 3, 2, 4).reshape(2, rows, PULSES)


def per_device(raw_echo, centroid, shifts, chirp_rate):
    devices = lax.axis_size("row")
    own_rows = raw_echo.shape[1] // devices
    blocks = raw_echo.reshape(2, devices, own_rows, raw_echo.shape[2])
    received = lax.all_to_all(arrange(blocks), "row", split_axis=0, concat_axis=0, tiled=True)

    def pick(values, device):
        block = jnp.clip(device, 0, devices - 1) * own_rows // BLOCK
        return jnp.sum(jnp.where(block == jnp.arange(values.shape[0], dtype=jnp.int32), values, 0))

    def exchange(up, down):
        up = from_behind(up, "row", -1)
        down = from_behind(down, "row", 1)
        return up, down

    device = lax.axis_index("row")
    centers = [pick(centroid, device + by) for by in (0, -1, 1)]
    return compute(received, exchange, *centers, pick(shifts, device), chirp_rate)


def solution(mesh):
    return jax.shard_map(
        per_device,
        mesh=mesh,
        in_specs=(P(None, "slab", "row"), P("slab"), P("slab"), P(("slab", "row"))),
        out_specs=P(None, ("slab", "row"), None),
        check_vma=False,
    )
```
